32 devices in a mesh: dp: 4 (over y, z), cp: 8 (over x, core).
Axes of the slice: x: 4, y: 2, z: 2, core: 2. Of those that a mesh axis runs over, the one named last changes fastest.
The devices are a block of a 4x4x8 slice.
Arguments:
- q_tok: bfloat16 [16384, 7, 128], P(('dp', 'cp')), parts along dimension 0
- k_tok: bfloat16 [16384, 128], P(('dp', 'cp')), parts along dimension 0
- v_tok: bfloat16 [16384, 128], P(('dp', 'cp')), parts along dimension 0
- fwd_out: bfloat16 [16384, 7, 128], P(('dp', 'cp')), parts along dimension 0
- d_out: bfloat16 [16384, 7, 128], P(('dp', 'cp')), parts along dimension 0
- lse_row: float32 [16384, 7], P(('dp', 'cp')), parts along dimension 0
Outputs:
- output 1: bfloat16 [16384, 7, 128], P(('dp', 'cp')), parts along dimension 0
- output 2: bfloat16 [16384, 128], P(('dp', 'cp')), parts along dimension 0
- output 3: bfloat16 [16384, 128], P(('dp', 'cp')), parts along dimension 0
There are 4 independent parts. The reference program is written for one: setup_inputs(seed, part) draws one part's arguments, and reference() takes and returns one part's arrays. A program takes and returns all parts, laid end to end along the dimension named above; each array names one.
All inputs are finite; a program needn't handle non-finite values.
Results may differ from the reference program's by a relative error of at most 0.001.
Values are sent between devices in bfloat16 or wider.
A program may use at most 768 MiB of HBM per device.

```python
import jax
import jax.numpy as jnp
from jax import lax

TOK_DEV = 512
CP = 8
GQA = 7
HEAD = 128

SEQ = CP * TOK_DEV
Q_BLOCK = min(TOK_DEV, 128)
SOFTMAX_SCALE = HEAD ** -0.5
GRAD_GAIN = 0.25 * SEQ ** 0.5


def attention_forward(q_tok, k_tok, v_tok):
    k_full = k_tok.astype(jnp.float32)
    v_full = v_tok.astype(jnp.float32)
    columns = jnp.arange(SEQ)
    n_blocks = SEQ // Q_BLOCK

    def one_block(block_in):
        q_block, row_ids = block_in
        logits = jnp.einsum('rgd,cd->rgc', q_block.astype(jnp.float32), k_full) * SOFTMAX_SCALE
        allowed = columns[None, :] <= row_ids[:, None]
        logits = jnp.where(allowed[:, None, :], logits, -jnp.inf)
        lse_block = jax.nn.logsumexp(logits, axis=-1)
        prob_mat = jnp.exp(logits - lse_block[:, :, None])
        out_block = jnp.einsum('rgc,cd->rgd', prob_mat, v_full)
        return out_block.astype(jnp.bfloat16), lse_block

    out_blocks, lse_blocks = lax.map(one_block, (q_tok.reshape(n_blocks, Q_BLOCK, GQA, HEAD), columns.reshape(n_blocks, Q_BLOCK)))
    return out_blocks.reshape(SEQ, GQA, HEAD), lse_blocks.reshape(SEQ, GQA)


def setup_inputs(seed: int = 0, part: int = 0) -> dict:
    base_key = jax.random.fold_in(jax.random.key(seed), part)
    key_q, key_k, key_v, key_m, key_g = jax.random.split(base_key, 5)
    q_tok = jax.random.normal(key_q, (SEQ, GQA, HEAD), jnp.float32).astype(jnp.bfloat16)
    k_tok = jax.random.normal(key_k, (SEQ, HEAD), jnp.float32).astype(jnp.bfloat16)
    v_mean = jax.random.normal(key_m, (HEAD,), jnp.float32)
    v_tok = (v_mean[None, :] + jax.random.normal(key_v, (SEQ, HEAD), jnp.float32)).astype(jnp.bfloat16)
    d_out = (GRAD_GAIN * jax.random.normal(key_g, (SEQ, GQA, HEAD), jnp.float32)).astype(jnp.bfloat16)
    fwd_out, lse_row = attention_forward(q_tok, k_tok, v_tok)
    return {'q_tok': q_tok, 'k_tok': k_tok, 'v_tok': v_tok, 'fwd_out': fwd_out, 'd_out': d_out, 'lse_row': lse_row}


def reference(q_tok, k_tok, v_tok, fwd_out, d_out, lse_row):
    row_delta = jnp.sum(d_out.astype(jnp.float32) * fwd_out.astype(jnp.float32), axis=-1)
    k_full = k_tok.astype(jnp.float32)
    v_full = v_tok.astype(jnp.float32)
    columns = jnp.arange(SEQ)
    n_blocks = SEQ // Q_BLOCK

    def one_block(carry, block_in):
        dk_acc, dv_acc = carry
        q_block, do_block, lse_block, delta_block, row_ids = block_in
        q_wide = q_block.astype(jnp.float32)
        do_wide = do_block.astype(jnp.float32)
        logits = jnp.einsum('rgd,cd->rgc', q_wide, k_full) * SOFTMAX_SCALE
        allowed = columns[None, :] <= row_ids[:, None]
        prob_mat = jnp.exp(jnp.where(allowed[:, None, :], logits - lse_block[:, :, None], -jnp.inf))
        d_prob = jnp.einsum('rgd,cd->rgc', do_wide, v_full)
        d_score = prob_mat * (d_prob - delta_block[:, :, None])
        prob_low = prob_mat.astype(jnp.bfloat16).astype(jnp.float32)
        score_low = d_score.astype(jnp.bfloat16).astype(jnp.float32)
        dq_block = jnp.einsum('rgc,cd->rgd', score_low, k_full) * SOFTMAX_SCALE
        dk_acc = dk_acc + jnp.einsum('rgc,rgd->cd', score_low, q_wide)
        dv_acc = dv_acc + jnp.einsum('rgc,rgd->cd', prob_low, do_wide)
        return (dk_acc, dv_acc), dq_block.astype(jnp.bfloat16)

    acc_start = (jnp.zeros((SEQ, HEAD), jnp.float32), jnp.zeros((SEQ, HEAD), jnp.float32))
    block_inputs = (q_tok.reshape(n_blocks, Q_BLOCK, GQA, HEAD), d_out.reshape(n_blocks, Q_BLOCK, GQA, HEAD), lse_row.reshape(n_blocks, Q_BLOCK, GQA), row_delta.reshape(n_blocks, Q_BLOCK, GQA), columns.reshape(n_blocks, Q_BLOCK))
    (dk_acc, dv_acc), dq_blocks = lax.scan(one_block, acc_start, block_inputs)
    grad_q = dq_blocks.reshape(SEQ, GQA, HEAD)
    grad_k = (dk_acc * SOFTMAX_SCALE).astype(jnp.bfloat16)
    grad_v = dv_acc.astype(jnp.bfloat16)
    return (grad_q, grad_k, grad_v)
```

```python
import functools

import jax
import jax.numpy as jnp
from jax import lax
from jax.experimental import pallas as pl
from jax.experimental.pallas import tpu as pltpu
from jax.sharding import PartitionSpec as P

LOG2E = 1.4426950408889634
MESH = pl.DeviceIdType.MESH
NT = ((1,), (1,))
NN = ((1,), (0,))


def dot(lhs, rhs, dims):
    return lax.dot_general(lhs, rhs, (dims, ((), ())), preferred_element_type=jnp.float32)


def wide(column, width):
    return jnp.concatenate([column] * (width // column.shape[1]), axis=1)


def attention_kernel(n_dev, softmax_scale, q_hbm, k_hbm, v_hbm, o_hbm, do_hbm, lse_hbm, dq_hbm, dk_hbm, dv_hbm,
                     q_ref, do_ref, o_ref, lse_ref, kv_ref, q_t, do_t, lse_col, delta_col, dq_acc, acc, p_buf, s_buf,
                     from_core, from_chip, dq_out, dkv_out,
                     load_sem, store_sem, kv_send, kv_recv, core_send, core_recv, chip_send, chip_recv):
    heads, rows, dim = q_ref.shape
    half = rows // 2
    n_chips = n_dev // 2
    me = lax.axis_index('cp')
    chip, core = me // 2, lax.rem(me, 2)
    partner = 2 * chip + 1 - core
    log_scale = softmax_scale * LOG2E

    barrier = pltpu.get_barrier_semaphore()
    for step in range(1, n_dev):
        pl.semaphore_signal(barrier, inc=1, device_id={'cp': lax.rem(me + step, n_dev)}, device_id_type=MESH)

    loads = [
        pltpu.make_async_copy(k_hbm, kv_ref.at[me, 0], load_sem.at[0]),
        pltpu.make_async_copy(v_hbm, kv_ref.at[me, 1], load_sem.at[1]),
        pltpu.make_async_copy(q_hbm, q_ref, load_sem.at[2]),
        pltpu.make_async_copy(do_hbm, do_ref, load_sem.at[3]),
        pltpu.make_async_copy(lse_hbm, lse_ref, load_sem.at[4]),
        pltpu.make_async_copy(o_hbm, o_ref, load_sem.at[5]),
    ]
    for load in loads:
        load.start()

    def remote(src, dst, send, recv, target):
        return pltpu.make_async_remote_copy(src_ref=src, dst_ref=dst, send_sem=send, recv_sem=recv, device_id={'cp': target}, device_id_type=MESH)

    def kv_to_chip(far):
        return remote(kv_ref.at[me], kv_ref.at[me], kv_send.at[far], kv_recv.at[me], me + 2 * far)

    def kv_to_partner():
        return remote(kv_ref.at[me], kv_ref.at[me], kv_send.at[0], kv_recv.at[me], partner)

    def kv_forward(stage):
        block = 2 * (chip - 1 - stage) + core
        return remote(kv_ref.at[block], kv_ref.at[block], kv_send.at[n_chips + stage], kv_recv.at[block], partner)

    def wait_kv(block):
        remote(kv_ref.at[block], kv_ref.at[block], kv_send.at[0], kv_recv.at[block], partner).wait_recv()

    def sum_to_partner(block, slot):
        return remote(acc.at[block], from_core.at[slot], core_send.at[slot], core_recv.at[slot], partner)

    def sum_to_owner(stage):
        block = 2 * (chip - 1 - stage) + core
        return remote(acc.at[block], from_chip.at[stage], chip_send.at[stage], chip_recv.at[stage], block)

    loads[0].wait()
    loads[1].wait()
    pl.semaphore_wait(barrier, n_dev - 1)
    for far in range(1, n_chips):
        @pl.when(chip + far < n_chips)
        def _():
            kv_to_chip(far).start()

    @pl.when(core == 0)
    def _():
        kv_to_partner().start()

    for load in loads[2:]:
        load.wait()

    def prepare(head):
        q_t[head] = q_ref[head].T
        do_t[head] = do_ref[head].T
        lse_col[head] = jnp.broadcast_to(lse_ref[pl.ds(head, 1), :] * LOG2E, (dim, rows)).T
        delta = jnp.sum(do_ref[head].astype(jnp.float32) * o_ref[head].astype(jnp.float32), axis=1, keepdims=True)
        delta_col[head] = jnp.broadcast_to(delta, (rows, dim))

    def tile(block, head, slot, row_at, col_at, diagonal):
        on_rows, on_cols = slice(row_at, rows), slice(col_at, col_at + half)
        prob = jnp.exp2(dot(q_ref[head, on_rows], kv_ref[block, 0, on_cols], NT) * log_scale - wide(lse_col[head, on_rows], half))
        if diagonal:
            row_ids = lax.broadcasted_iota(jnp.int32, prob.shape, 0)
            col_ids = lax.broadcasted_iota(jnp.int32, prob.shape, 1)
            prob = jnp.where(col_ids <= row_ids, prob, 0.0)
        d_prob = dot(do_ref[head, on_rows], kv_ref[block, 1, on_cols], NT)
        score = prob * (d_prob - wide(delta_col[head, on_rows], half))
        p_buf[slot, on_rows, on_cols] = prob.astype(jnp.bfloat16)
        s_buf[slot, on_rows, on_cols] = score.astype(jnp.bfloat16)

    def add_to(ref, index, value, first):
        if first:
            ref[index] = value
        else:
            ref[index] += value

    def own_block(block):
        for step in range(heads + 1):
            if step < heads:
                tile(block, step, step % 2, 0, 0, True)
                tile(block, step, step % 2, half, half, True)
            if step >= 1:
                head, slot = step - 1, (step - 1) % 2
                first = head == 0
                left, right, low = slice(0, half), slice(half, rows), slice(half, rows)
                add_to(acc, (block, 1, slice(None), left), dot(do_t[head], p_buf[slot, :, left], NN), first)
                add_to(acc, (block, 0, slice(None), left), dot(q_t[head], s_buf[slot, :, left], NN), first)
                add_to(acc, (block, 1, slice(None), right), dot(do_t[head, :, low], p_buf[slot, low, right], NN), first)
                add_to(acc, (block, 0, slice(None), right), dot(q_t[head, :, low], s_buf[slot, low, right], NN), first)
                dq_acc[head, left] = dot(s_buf[slot, left, left], kv_ref[block, 0, left], NN)
                dq_acc[head, low] = dot(s_buf[slot, low, :], kv_ref[block, 0], NN)

    def full_block(block):
        for step in range(heads + 1):
            if step < heads:
                tile(block, step, step % 2, 0, 0, False)
                tile(block, step, step % 2, 0, half, False)
            if step >= 1:
                head, slot = step - 1, (step - 1) % 2
                prob, score = p_buf[slot], s_buf[slot]
                add_to(acc, (block, 1), dot(do_t[head], prob, NN), head == 0)
                add_to(acc, (block, 0), dot(q_t[head], score, NN), head == 0)
                dq_acc[head] += dot(score, kv_ref[block, 0], NN)

    def prepare_one(head, _):
        prepare(head)
        return 0

    lax.fori_loop(0, heads, prepare_one, 0)
    own_block(me)

    def merge(stage):
        block = 2 * (chip - 1 - stage) + core
        sum_to_partner(block, stage).wait_recv()
        acc[block] += from_core[stage]
        sum_to_owner(stage).start()

    def visit(turn, _):
        stage, second = turn // 2, lax.rem(turn, 2)
        is_local = turn == 2 * chip
        mine = jnp.logical_and(jnp.logical_not(is_local), (turn == 0) | ((second == 1) & (stage >= 1)))
        parity = jnp.where(mine, core, 1 - core)
        block = jnp.where(is_local, 2 * chip, 2 * (chip - 1 - stage) + parity)

        ahead = (turn + 1) // 2

        @pl.when(((turn == 0) | (second == 1)) & (ahead < chip))
        def _():
            wait_kv(2 * (chip - 1 - ahead) + core)
            kv_forward(ahead).start()

        @pl.when(jnp.logical_not(mine))
        def _():
            wait_kv(block)

        full_block(block)

        @pl.when(jnp.logical_not(mine))
        def _():
            sum_to_partner(block, jnp.where(is_local, n_chips - 1, stage)).start()

        @pl.when((turn == 2) & (chip >= 2))
        def _():
            merge(0)

        @pl.when((turn == 1) & (chip == 1))
        def _():
            merge(0)

        @pl.when((second == 1) & (stage >= 1))
        def _():
            merge(stage)

        return 0

    lax.fori_loop(0, me, visit, 0)

    for head in range(heads):
        dq_out[head] = (dq_acc[head] * softmax_scale).astype(jnp.bfloat16)
    store_dq = pltpu.make_async_copy(dq_out, dq_hbm, store_sem.at[0])
    store_dq.start()

    @pl.when(core == 0)
    def _():
        sum_to_partner(me, n_chips - 1).wait_recv()
        acc[me] += from_core[n_chips - 1]

    for far in range(1, n_chips):
        @pl.when(chip + far < n_chips)
        def _():
            remote(acc.at[me], from_chip.at[far - 1], chip_send.at[far - 1], chip_recv.at[far - 1], partner).wait_recv()
            acc[me] += from_chip[far - 1]

    dkv_out[0] = (acc[me, 0] * softmax_scale).T.astype(jnp.bfloat16)
    store_dk = pltpu.make_async_copy(dkv_out.at[0], dk_hbm, store_sem.at[1])
    store_dk.start()
    dkv_out[1] = acc[me, 1].T.astype(jnp.bfloat16)
    store_dv = pltpu.make_async_copy(dkv_out.at[1], dv_hbm, store_sem.at[2])
    store_dv.start()

    for far in range(1, n_chips):
        @pl.when(chip + far < n_chips)
        def _():
            kv_to_chip(far).wait_send()

    @pl.when(core == 0)
    def _():
        kv_to_partner().wait_send()

    @pl.when(core == 1)
    def _():
        sum_to_partner(2 * chip, n_chips - 1).wait_send()

    def finish(stage, _):
        kv_forward(stage).wait_send()
        sum_to_partner(2 * (chip - 1 - stage) + 1 - core, stage).wait_send()
        sum_to_owner(stage).wait_send()
        return 0

    lax.fori_loop(0, chip, finish, 0)
    store_dq.wait()
    store_dk.wait()
    store_dv.wait()


def solution(mesh):
    n_dev = mesh.shape['cp']
    n_chips = n_dev // 2
    row_spec = P(('dp', 'cp'))
    f32, bf16 = jnp.float32, jnp.bfloat16

    def local_fn(q_tok, k_tok, v_tok, fwd_out, d_out, lse_row):
        rows, heads, dim = q_tok.shape
        per_head = (heads, rows, dim)
        in_hbm = pl.BlockSpec(memory_space=pl.ANY)
        dma = pltpu.SemaphoreType.DMA
        grad_q, grad_k, grad_v = pl.pallas_call(
            functools.partial(attention_kernel, n_dev, dim ** -0.5),
            out_shape=(
                jax.ShapeDtypeStruct(per_head, bf16),
                jax.ShapeDtypeStruct((rows, dim), bf16),
                jax.ShapeDtypeStruct((rows, dim), bf16),
            ),
            in_specs=[in_hbm] * 6,
            out_specs=(in_hbm, in_hbm, in_hbm),
            scratch_shapes=[
                pltpu.VMEM(per_head, bf16),
                pltpu.VMEM(per_head, bf16),
                pltpu.VMEM(per_head, bf16),
                pltpu.VMEM((heads, rows), f32),
                pltpu.VMEM((n_dev, 2, rows, dim), bf16),
                pltpu.VMEM((heads, dim, rows), bf16),
                pltpu.VMEM((heads, dim, rows), bf16),
                pltpu.VMEM(per_head, f32),
                pltpu.VMEM(per_head, f32),
                pltpu.VMEM(per_head, f32),
                pltpu.VMEM((n_dev, 2, dim, rows), f32),
                pltpu.VMEM((2, rows, rows), bf16),
                pltpu.VMEM((2, rows, rows), bf16),
                pltpu.VMEM((n_chips, 2, dim, rows), f32),
                pltpu.VMEM((n_chips - 1, 2, dim, rows), f32),
                pltpu.VMEM(per_head, bf16),
                pltpu.VMEM((2, rows, dim), bf16),
                dma((6,)),
                dma((3,)),
                dma((2 * n_chips,)),
                dma((n_dev,)),
                dma((n_chips,)),
                dma((n_chips,)),
                dma((n_chips - 1,)),
                dma((n_chips - 1,)),
            ],
            compiler_params=pltpu.CompilerParams(collective_id=0, has_side_effects=True),
            name='attention_grad',
        )(q_tok.transpose(1, 0, 2), k_tok, v_tok, fwd_out.transpose(1, 0, 2), d_out.transpose(1, 0, 2), lse_row.T)
        return grad_q.transpose(1, 0, 2), grad_k, grad_v

    return jax.shard_map(local_fn, mesh=mesh, in_specs=(row_spec,) * 6, out_specs=(row_spec,) * 3, check_vma=False)
```

```python
import functools

import jax
import jax.numpy as jnp
from jax import lax
from jax.experimental import pallas as pl
from jax.experimental.pallas import tpu as pltpu
from jax.sharding import PartitionSpec as P

LOG2E = 1.4426950408889634
MESH = pl.DeviceIdType.MESH
NT = ((1,), (1,))
NN = ((1,), (0,))


def dot(lhs, rhs, dims):
    return lax.dot_general(lhs, rhs, (dims, ((), ())), preferred_element_type=jnp.float32)


def wide(column, width):
    return jnp.concatenate([column] * (width // column.shape[1]), axis=1)


def attention_kernel(n_dev, softmax_scale, q_hbm, k_hbm, v_hbm, o_hbm, do_hbm, lse_hbm, dq_ref, dk_ref, dv_ref,
                     q_ref, do_ref, o_ref, lse_ref, kv_ref, q_t, do_t, lse_col, delta_col, dq_acc, acc, p_buf, s_buf,
                     from_core, from_chip,
                     load_sem, own_send, forward_send, kv_recv, core_send, core_recv, chip_send, chip_recv):
    heads, rows, dim = q_ref.shape
    half = rows // 2
    n_chips = n_dev // 2
    local = n_chips - 1
    me = lax.axis_index('cp')
    chip, core = me // 2, lax.rem(me, 2)
    partner = 2 * chip + 1 - core
    log_scale = softmax_scale * LOG2E

    barrier = pltpu.get_barrier_semaphore()
    for step in range(1, n_dev):
        pl.semaphore_signal(barrier, inc=1, device_id={'cp': lax.rem(me + step, n_dev)}, device_id_type=MESH)

    kv_loads = []
    for part in range(2):
        on_part = pl.ds(part * half, half)
        kv_loads.append(pltpu.make_async_copy(k_hbm.at[on_part], kv_ref.at[me, part, 0], load_sem.at[2 * part]))
        kv_loads.append(pltpu.make_async_copy(v_hbm.at[on_part], kv_ref.at[me, part, 1], load_sem.at[2 * part + 1]))
    loads = [
        pltpu.make_async_copy(q_hbm, q_ref, load_sem.at[4]),
        pltpu.make_async_copy(do_hbm, do_ref, load_sem.at[5]),
        pltpu.make_async_copy(lse_hbm, lse_ref, load_sem.at[6]),
        pltpu.make_async_copy(o_hbm, o_ref, load_sem.at[7]),
    ]
    for load in kv_loads + loads:
        load.start()

    def remote(src, dst, send, recv, target):
        return pltpu.make_async_remote_copy(src_ref=src, dst_ref=dst, send_sem=send, recv_sem=recv, device_id={'cp': target}, device_id_type=MESH)

    def owner_chip(stage):
        return jnp.where((chip == n_chips - 1) & (stage < 2), 1 - stage, stage)

    def kv_to_chip(far, part):
        return remote(kv_ref.at[me, part], kv_ref.at[me, part], own_send.at[far, part], kv_recv.at[me, part], me + 2 * far)

    def kv_to_partner(part):
        return remote(kv_ref.at[me, part], kv_ref.at[me, part], own_send.at[0, part], kv_recv.at[me, part], partner)

    def kv_forward(stage, part):
        block = 2 * owner_chip(stage) + core
        return remote(kv_ref.at[block, part], kv_ref.at[block, part], forward_send.at[stage, part], kv_recv.at[block, part], partner)

    def wait_kv(block, part):
        remote(kv_ref.at[block, part], kv_ref.at[block, part], own_send.at[0, part], kv_recv.at[block, part], partner).wait_recv()

    def receive(stage, part):
        wait_kv(2 * owner_chip(stage) + core, part)
        kv_forward(stage, part).start()

    def sum_to_partner(block, slot, part):
        return remote(acc.at[block, part], from_core.at[slot, part], core_send.at[slot, part], core_recv.at[slot, part], partner)

    def sum_to_owner(stage, part):
        owner = owner_chip(stage)
        block, slot = 2 * owner + core, chip - owner - 1
        return remote(acc.at[block, part], from_chip.at[slot, part], chip_send.at[stage, part], chip_recv.at[slot, part], block)

    def merge(stage, part):
        block = 2 * owner_chip(stage) + core
        sum_to_partner(block, stage, part).wait_recv()
        acc[block, part] += from_core[stage, part]
        sum_to_owner(stage, part).start()

    def on_later_chips(action, fars):
        for far in fars:
            @pl.when(chip + far < n_chips)
            def _():
                for part in range(2):
                    action(far, part)

    for load in kv_loads:
        load.wait()
    pl.semaphore_wait(barrier, n_dev - 1)
    on_later_chips(lambda far, part: kv_to_chip(far, part).start(), range(n_chips - 2, 0, -1))

    @pl.when(core == 0)
    def _():
        for part in range(2):
            kv_to_partner(part).start()

    for load in loads:
        load.wait()

    def prepare(head, _):
        q_t[head] = q_ref[head].T
        do_t[head] = do_ref[head].T
        lse_col[head] = jnp.broadcast_to(lse_ref[pl.ds(head, 1), :] * LOG2E, (dim, rows)).T
        delta = jnp.sum(do_ref[head].astype(jnp.float32) * o_ref[head].astype(jnp.float32), axis=1, keepdims=True)
        delta_col[head] = jnp.broadcast_to(delta, (rows, dim))
        return 0

    lax.fori_loop(0, heads, prepare, 0)

    def tile(block, part, head, slot, row_at, col_at, diagonal):
        on_rows, on_cols = slice(row_at, rows), slice(col_at, col_at + half)
        prob = jnp.exp2(dot(q_ref[head, on_rows], kv_ref[block, part, 0], NT) * log_scale - wide(lse_col[head, on_rows], half))
        if diagonal:
            row_ids = lax.broadcasted_iota(jnp.int32, prob.shape, 0)
            col_ids = lax.broadcasted_iota(jnp.int32, prob.shape, 1)
            prob = jnp.where(col_ids <= row_ids, prob, 0.0)
        d_prob = dot(do_ref[head, on_rows], kv_ref[block, part, 1], NT)
        score = prob * (d_prob - wide(delta_col[head, on_rows], half))
        p_buf[slot, on_rows, on_cols] = prob.astype(jnp.bfloat16)
        s_buf[slot, on_rows, on_cols] = score.astype(jnp.bfloat16)

    def add_to(ref, index, value, first):
        if first:
            ref[index] = value
        else:
            ref[index] += value

    def add_sums(block, part, head, slot, row_at, col_at):
        on_rows, on_cols = slice(row_at, rows), slice(col_at, col_at + half)
        add_to(acc, (block, part, 1), dot(do_t[head, :, on_rows], p_buf[slot, on_rows, on_cols], NN), head == 0)
        add_to(acc, (block, part, 0), dot(q_t[head, :, on_rows], s_buf[slot, on_rows, on_cols], NN), head == 0)

    def keys(block):
        return jnp.concatenate([kv_ref[block, 0, 0], kv_ref[block, 1, 0]], axis=0)

    def staggered(make, use):
        for step in range(heads + 1):
            if step < heads:
                make(step, step % 2)
            if step >= 1:
                use(step - 1, (step - 1) % 2)

    def own_block(block):
        def make(head, slot):
            tile(block, 0, head, slot, 0, 0, True)
            tile(block, 1, head, slot, half, half, True)

        def use(head, slot):
            add_sums(block, 0, head, slot, 0, 0)
            add_sums(block, 1, head, slot, half, half)
            dq_acc[head, 0:half] = dot(s_buf[slot, 0:half, 0:half], kv_ref[block, 0, 0], NN)
            dq_acc[head, half:rows] = dot(s_buf[slot, half:rows, :], keys(block), NN)

        staggered(make, use)

    def full_block(block):
        def make(head, slot):
            tile(block, 0, head, slot, 0, 0, False)
            tile(block, 1, head, slot, 0, half, False)

        def use(head, slot):
            add_sums(block, 0, head, slot, 0, 0)
            add_sums(block, 1, head, slot, 0, half)
            dq_acc[head] += dot(s_buf[slot], keys(block), NN)

        staggered(make, use)

    def half_block(block, part):
        def make(head, slot):
            tile(block, part, head, slot, 0, 0, False)

        def use(head, slot):
            add_sums(block, part, head, slot, 0, 0)
            dq_acc[head] += dot(s_buf[slot, :, 0:half], kv_ref[block, part, 0], NN)

        staggered(make, use)

    own_block(me)
    on_later_chips(lambda far, part: kv_to_chip(far, part).start(), [n_chips - 1])

    def visit(turn, _):
        stage, quarter = turn // 4, lax.rem(turn, 4)
        part, odd = quarter // 2, lax.rem(quarter, 2)
        mine = jnp.where(stage == 0, 1 - odd, odd)
        block = 2 * owner_chip(stage) + jnp.where(mine == 1, core, 1 - core)

        @pl.when((stage == 0) & (odd == 0))
        def _():
            receive(0, part)

        @pl.when((quarter == 3) & (stage + 1 < chip))
        def _():
            receive(stage + 1, 0)

        @pl.when((quarter == 1) & (stage >= 1))
        def _():
            receive(stage, 1)

        @pl.when(mine == 0)
        def _():
            wait_kv(block, part)

        half_block(block, part)

        @pl.when(mine == 0)
        def _():
            sum_to_partner(block, stage, part).start()

        @pl.when((stage == 0) & (quarter == 2))
        def _():
            merge(0, 0)

        @pl.when(((stage == 0) & (quarter == 3) & (chip == 1)) | ((stage == 1) & (quarter == 0)))
        def _():
            merge(0, 1)

        @pl.when((stage >= 1) & (odd == 1))
        def _():
            merge(stage, part)

        return 0

    lax.fori_loop(0, 4 * chip, visit, 0)

    @pl.when(core == 1)
    def _():
        for part in range(2):
            wait_kv(2 * chip, part)
        full_block(2 * chip)
        for part in range(2):
            sum_to_partner(2 * chip, local, part).start()

    for head in range(heads):
        dq_ref[head] = (dq_acc[head] * softmax_scale).astype(jnp.bfloat16)

    @pl.when(core == 0)
    def _():
        for part in range(2):
            sum_to_partner(me, local, part).wait_recv()
        acc[me] += from_core[local]

    def collect(far, part):
        remote(acc.at[me, part], from_chip.at[far - 1, part], chip_send.at[far - 1, part], chip_recv.at[far - 1, part], partner).wait_recv()
        acc[me, part] += from_chip[far - 1, part]

    on_later_chips(collect, range(1, n_chips))
    for part in range(2):
        on_part = slice(part * half, (part + 1) * half)
        dk_ref[on_part] = (acc[me, part, 0] * softmax_scale).T.astype(jnp.bfloat16)
        dv_ref[on_part] = acc[me, part, 1].T.astype(jnp.bfloat16)

    on_later_chips(lambda far, part: kv_to_chip(far, part).wait_send(), range(1, n_chips))

    @pl.when(core == 0)
    def _():
        for part in range(2):
            kv_to_partner(part).wait_send()

    @pl.when(core == 1)
    def _():
        for part in range(2):
            sum_to_partner(2 * chip, local, part).wait_send()

    def finish(stage, _):
        for part in range(2):
            kv_forward(stage, part).wait_send()
            sum_to_partner(2 * owner_chip(stage) + 1 - core, stage, part).wait_send()
            sum_to_owner(stage, part).wait_send()
        return 0

    lax.fori_loop(0, chip, finish, 0)


def store_kernel(dq_ref, dk_ref, dv_ref, dq_hbm, dk_hbm, dv_hbm, sem):
    stores = [
        pltpu.make_async_copy(dq_ref, dq_hbm, sem.at[0]),
        pltpu.make_async_copy(dk_ref, dk_hbm, sem.at[1]),
        pltpu.make_async_copy(dv_ref, dv_hbm, sem.at[2]),
    ]
    for store in stores:
        store.start()
    for store in stores:
        store.wait()


def solution(mesh):
    n_dev = mesh.shape['cp']
    n_chips = n_dev // 2
    row_spec = P(('dp', 'cp'))
    f32, bf16 = jnp.float32, jnp.bfloat16

    def local_fn(q_tok, k_tok, v_tok, fwd_out, d_out, lse_row):
        rows, heads, dim = q_tok.shape
        half = rows // 2
        per_head = (heads, rows, dim)
        anywhere = pl.BlockSpec(memory_space=pl.ANY)
        in_vmem = pl.BlockSpec(memory_space=pltpu.VMEM)
        dma = pltpu.SemaphoreType.DMA
        operands = (q_tok.transpose(1, 0, 2), k_tok, v_tok, fwd_out.transpose(1, 0, 2), d_out.transpose(1, 0, 2), lse_row.T)
        grads = pl.pallas_call(
            functools.partial(attention_kernel, n_dev, dim ** -0.5),
            out_shape=(pltpu.VMEM(per_head, bf16), pltpu.VMEM((rows, dim), bf16), pltpu.VMEM((rows, dim), bf16)),
            in_specs=[anywhere] * 6,
            out_specs=(in_vmem, in_vmem, in_vmem),
            scratch_shapes=[
                pltpu.VMEM(per_head, bf16),
                pltpu.VMEM(per_head, bf16),
                pltpu.VMEM(per_head, bf16),
                pltpu.VMEM((heads, rows), f32),
                pltpu.VMEM((n_dev, 2, 2, half, dim), bf16),
                pltpu.VMEM((heads, dim, rows), bf16),
                pltpu.VMEM((heads, dim, rows), bf16),
                pltpu.VMEM(per_head, f32),
                pltpu.VMEM(per_head, f32),
                pltpu.VMEM(per_head, f32),
                pltpu.VMEM((n_dev, 2, 2, dim, half), f32),
                pltpu.VMEM((2, rows, rows), bf16),
                pltpu.VMEM((2, rows, rows), bf16),
                pltpu.VMEM((n_chips, 2, 2, dim, half), f32),
                pltpu.VMEM((n_chips - 1, 2, 2, dim, half), f32),
                dma((8,)),
                dma((n_chips, 2)),
                dma((n_chips - 1, 2)),
                dma((n_dev, 2)),
                dma((n_chips, 2)),
                dma((n_chips, 2)),
                dma((n_chips - 1, 2)),
                dma((n_chips - 1, 2)),
            ],
            compiler_params=pltpu.CompilerParams(collective_id=0, has_side_effects=True, vmem_limit_bytes=40 * 2**20),
            name='attention_grad',
        )(*[pltpu.with_memory_space_constraint(operand, pltpu.HBM) for operand in operands])
        grad_q, grad_k, grad_v = pl.pallas_call(
            store_kernel,
            out_shape=[jax.ShapeDtypeStruct(grad.shape, bf16) for grad in grads],
            in_specs=[in_vmem] * 3,
            out_specs=[anywhere] * 3,
            scratch_shapes=[dma((3,))],
            compiler_params=pltpu.CompilerParams(vmem_limit_bytes=2**20),
            name='store_grads',
        )(*grads)
        return grad_q.transpose(1, 0, 2), grad_k, grad_v

    return jax.shard_map(local_fn, mesh=mesh, in_specs=(row_spec,) * 6, out_specs=(row_spec,) * 3, check_vma=False)
```

```python
import functools

import jax
import jax.numpy as jnp
from jax import lax
from jax.experimental import pallas as pl
from jax.experimental.pallas import tpu as pltpu
from jax.sharding import PartitionSpec as P

LOG2E = 1.4426950408889634
MESH = pl.DeviceIdType.MESH
NT = ((1,), (1,))
NN = ((1,), (0,))


def dot(lhs, rhs, dims):
    return lax.dot_general(lhs, rhs, (dims, ((), ())), preferred_element_type=jnp.float32)


def wide(column, width):
    return jnp.concatenate([column] * (width // column.shape[1]), axis=1)


def attention_kernel(n_dev, softmax_scale, q_hbm, k_hbm, v_hbm, o_hbm, do_hbm, lse_hbm, dq_ref, dk_ref, dv_ref,
                     q_ref, do_ref, o_ref, lse_ref, kv_ref, q_t, do_t, lse_col, delta_col, dq_acc, acc, p_buf, s_buf,
                     from_core, from_chip,
                     load_sem, own_send, forward_send, kv_recv, core_send, core_recv, chip_send, chip_recv):
    heads, rows, dim = q_ref.shape
    half = rows // 2
    n_chips = n_dev // 2
    local = n_chips - 1
    me = lax.axis_index('cp')
    chip, core = me // 2, lax.rem(me, 2)
    partner = 2 * chip + 1 - core
    log_scale = softmax_scale * LOG2E

    barrier = pltpu.get_barrier_semaphore()
    for step in range(1, n_dev):
        pl.semaphore_signal(barrier, inc=1, device_id={'cp': lax.rem(me + step, n_dev)}, device_id_type=MESH)

    kv_loads = []
    for part in range(2):
        on_part = pl.ds(part * half, half)
        kv_loads.append(pltpu.make_async_copy(k_hbm.at[on_part], kv_ref.at[me, part, 0], load_sem.at[2 * part]))
        kv_loads.append(pltpu.make_async_copy(v_hbm.at[on_part], kv_ref.at[me, part, 1], load_sem.at[2 * part + 1]))
    early = heads // 3

    def head_loads(at, count, sem):
        on_heads = pl.ds(at, count)
        pairs = ((q_hbm, q_ref), (do_hbm, do_ref), (o_hbm, o_ref))
        return [pltpu.make_async_copy(src.at[on_heads], dst.at[on_heads], load_sem.at[sem + n]) for n, (src, dst) in enumerate(pairs)]

    first_loads = [pltpu.make_async_copy(lse_hbm, lse_ref, load_sem.at[4])] + head_loads(0, early, 5)
    later_loads = head_loads(early, heads - early, 8)
    for load in kv_loads + first_loads + later_loads:
        load.start()

    def remote(src, dst, send, recv, target):
        return pltpu.make_async_remote_copy(src_ref=src, dst_ref=dst, send_sem=send, recv_sem=recv, device_id={'cp': target}, device_id_type=MESH)

    def round_of(turn, side):
        late, odd = turn // 2, lax.rem(turn, 2)
        flip = jnp.where(turn == 4, side, 1 - side)
        last_owner = jnp.where(turn == 0, 2, jnp.where(turn < 3, 1, jnp.where(turn == 3, 0, 2 * flip)))
        last_part = jnp.where((turn == 2) | (turn >= 4), 1, 0)
        is_last = chip == n_chips - 1
        return jnp.where(is_last, last_owner, late), jnp.where(is_last, last_part, odd)

    def kv_to_chip(far, part):
        return remote(kv_ref.at[me, part], kv_ref.at[me, part], own_send.at[far, part], kv_recv.at[me, part], me + 2 * far)

    def kv_to_partner(part):
        return remote(kv_ref.at[me, part], kv_ref.at[me, part], own_send.at[0, part], kv_recv.at[me, part], partner)

    def kv_forward(owner, part):
        block = 2 * owner + core
        return remote(kv_ref.at[block, part], kv_ref.at[block, part], forward_send.at[owner, part], kv_recv.at[block, part], partner)

    def wait_kv(block, part):
        remote(kv_ref.at[block, part], kv_ref.at[block, part], own_send.at[0, part], kv_recv.at[block, part], partner).wait_recv()

    def receive(turn):
        owner, part = round_of(turn, core)
        wait_kv(2 * owner + core, part)
        kv_forward(owner, part).start()

    def sum_to_partner(block, slot, part):
        return remote(acc.at[block, part], from_core.at[slot, part], core_send.at[slot, part], core_recv.at[slot, part], partner)

    def sum_to_owner(owner, part):
        block, slot = 2 * owner + core, chip - owner - 1
        target = jnp.where(slot == 1, 2 * (2 * n_chips - 3 - chip) + core, block)
        return remote(acc.at[block, part], from_chip.at[slot, part], chip_send.at[owner, part], chip_recv.at[slot, part], target)

    def wait_sum(slot, part):
        remote(acc.at[me, part], from_chip.at[slot, part], chip_send.at[0, part], chip_recv.at[slot, part], partner).wait_recv()

    def merge(turn):
        owner, part = round_of(turn, core)
        block = 2 * owner + core
        sum_to_partner(block, owner, part).wait_recv()
        acc[block, part] += from_core[owner, part]

        @pl.when((chip >= 2) & (chip + owner == n_chips - 1))
        def _():
            wait_sum(1, part)
            acc[block, part] += from_chip[1, part]

        sum_to_owner(owner, part).start()

    def on_later_chips(action, fars):
        for far in fars:
            @pl.when(chip + far < n_chips)
            def _():
                for part in range(2):
                    action(far, part)

    for load in kv_loads:
        load.wait()
    pl.semaphore_wait(barrier, n_dev - 1)
    on_later_chips(lambda far, part: kv_to_chip(far, part).start(), range(n_chips - 2, 0, -1))

    @pl.when(core == 0)
    def _():
        for part in range(2):
            kv_to_partner(part).start()

    for load in first_loads:
        load.wait()

    def prepare(head):
        if head == early:
            for load in later_loads:
                load.wait()
        at = head + me // n_dev
        q_t[at] = q_ref[head].T
        do_t[at] = do_ref[head].T
        lse_col[at] = jnp.broadcast_to(lse_ref[pl.ds(at, 1), :] * LOG2E, (dim, rows)).T
        delta = jnp.sum(do_ref[head].astype(jnp.float32) * o_ref[head].astype(jnp.float32), axis=1, keepdims=True)
        delta_col[at] = jnp.broadcast_to(delta, (rows, dim))

    def tile(block, part, head, slot, row_at, col_at, diagonal):
        on_rows, on_cols = slice(row_at, rows), slice(col_at, col_at + half)
        prob = jnp.exp2(dot(q_ref[head, on_rows], kv_ref[block, part, 0], NT) * log_scale - wide(lse_col[head, on_rows], half))
        if diagonal:
            row_ids = lax.broadcasted_iota(jnp.int32, prob.shape, 0)
            col_ids = lax.broadcasted_iota(jnp.int32, prob.shape, 1)
            prob = jnp.where(col_ids <= row_ids, prob, 0.0)
        d_prob = dot(do_ref[head, on_rows], kv_ref[block, part, 1], NT)
        score = prob * (d_prob - wide(delta_col[head, on_rows], half))
        p_buf[slot, on_rows, on_cols] = prob.astype(jnp.bfloat16)
        s_buf[slot, on_rows, on_cols] = score.astype(jnp.bfloat16)

    def add_to(ref, index, value, first):
        if first:
            ref[index] = value
        else:
            ref[index] += value

    def add_sums(block, part, head, slot, row_at, col_at):
        on_rows, on_cols = slice(row_at, rows), slice(col_at, col_at + half)
        add_to(acc, (block, part, 1), dot(do_t[head, :, on_rows], p_buf[slot, on_rows, on_cols], NN), head == 0)
        add_to(acc, (block, part, 0), dot(q_t[head, :, on_rows], s_buf[slot, on_rows, on_cols], NN), head == 0)

    def keys(block):
        return jnp.concatenate([kv_ref[block, 0, 0], kv_ref[block, 1, 0]], axis=0)

    def staggered(make, use):
        for step in range(heads + 1):
            if step < heads:
                make(step, step % 2)
            if step >= 1:
                use(step - 1, (step - 1) % 2)

    def own_block(block):
        def make(head, slot):
            tile(block, 0, head, slot, 0, 0, True)
            tile(block, 1, head, slot, half, half, True)
            if head + 1 < heads:
                prepare(head + 1)

        def use(head, slot):
            add_sums(block, 0, head, slot, 0, 0)
            add_sums(block, 1, head, slot, half, half)
            dq_acc[head, 0:half] = dot(s_buf[slot, 0:half, 0:half], kv_ref[block, 0, 0], NN)
            dq_acc[head, half:rows] = dot(s_buf[slot, half:rows, :], keys(block), NN)

        prepare(0)
        staggered(make, use)

    def half_block(block, part):
        def make(head, slot):
            tile(block, part, head, slot, 0, 0, False)

        def use(head, slot):
            add_sums(block, part, head, slot, 0, 0)
            dq_acc[head] += dot(s_buf[slot, :, 0:half], kv_ref[block, part, 0], NN)

        staggered(make, use)

    own_block(me)
    on_later_chips(lambda far, part: kv_to_chip(far, part).start(), [n_chips - 1])

    def core_block(part):
        wait_kv(2 * chip, part)
        half_block(2 * chip, part)
        sum_to_partner(2 * chip, local, part).start()

    def visit(visit_id, _):
        turn, second = visit_id // 2, lax.rem(visit_id, 2)
        mine = jnp.where(turn < 2, 1 - second, second)
        side = jnp.where(mine == 1, core, 1 - core)
        owner, part = round_of(turn, side)
        block = 2 * owner + side

        @pl.when((turn < 2) & (second == 0))
        def _():
            receive(turn)

        @pl.when((turn >= 1) & (second == 1) & (turn + 1 < 2 * chip))
        def _():
            receive(turn + 1)

        @pl.when(mine == 0)
        def _():
            wait_kv(block, part)

        half_block(block, part)

        @pl.when(mine == 0)
        def _():
            sum_to_partner(block, owner, part).start()

        @pl.when((turn >= 1) & (turn <= 3) & (second == 0))
        def _():
            merge(turn - 1)

        @pl.when((second == 1) & ((turn >= 3) | ((turn == 1) & (chip == 1))))
        def _():
            merge(turn)

        return 0

    lax.fori_loop(0, 4 * chip, visit, 0)

    @pl.when(core == 1)
    def _():
        core_block(0)
        core_block(1)

    for head in range(heads):
        dq_ref[head] = (dq_acc[head] * softmax_scale).astype(jnp.bfloat16)

    @pl.when(core == 0)
    def _():
        for part in range(2):
            sum_to_partner(me, local, part).wait_recv()
        acc[me] += from_core[local]

    for part in range(2):
        on_part = slice(part * half, (part + 1) * half)
        for far in (1, n_chips - 1):
            @pl.when(chip + far < n_chips)
            def _():
                wait_sum(far - 1, part)
                acc[me, part] += from_chip[far - 1, part]

        dk_ref[on_part] = (acc[me, part, 0] * softmax_scale).T.astype(jnp.bfloat16)
        dv_ref[on_part] = acc[me, part, 1].T.astype(jnp.bfloat16)

    on_later_chips(lambda far, part: kv_to_chip(far, part).wait_send(), range(1, n_chips))

    @pl.when(core == 0)
    def _():
        for part in range(2):
            kv_to_partner(part).wait_send()

    @pl.when(core == 1)
    def _():
        for part in range(2):
            sum_to_partner(2 * chip, local, part).wait_send()

    def finish(owner, _):
        for part in range(2):
            kv_forward(owner, part).wait_send()
            sum_to_partner(2 * owner + 1 - core, owner, part).wait_send()
            sum_to_owner(owner, part).wait_send()
        return 0

    lax.fori_loop(0, chip, finish, 0)


def store_kernel(dq_ref, dk_ref, dv_ref, dq_hbm, dk_hbm, dv_hbm, sem):
    stores = [
        pltpu.make_async_copy(dq_ref, dq_hbm, sem.at[0]),
        pltpu.make_async_copy(dk_ref, dk_hbm, sem.at[1]),
        pltpu.make_async_copy(dv_ref, dv_hbm, sem.at[2]),
    ]
    for store in stores:
        store.start()
    for store in stores:
        store.wait()


def solution(mesh):
    n_dev = mesh.shape['cp']
    n_chips = n_dev // 2
    row_spec = P(('dp', 'cp'))
    f32, bf16 = jnp.float32, jnp.bfloat16

    def local_fn(q_tok, k_tok, v_tok, fwd_out, d_out, lse_row):
        rows, heads, dim = q_tok.shape
        half = rows // 2
        per_head = (heads, rows, dim)
        anywhere = pl.BlockSpec(memory_space=pl.ANY)
        in_vmem = pl.BlockSpec(memory_space=pltpu.VMEM)
        dma = pltpu.SemaphoreType.DMA
        operands = (q_tok.transpose(1, 0, 2), k_tok, v_tok, fwd_out.transpose(1, 0, 2), d_out.transpose(1, 0, 2), lse_row.T)
        grads = pl.pallas_call(
            functools.partial(attention_kernel, n_dev, dim ** -0.5),
            out_shape=(pltpu.VMEM(per_head, bf16), pltpu.VMEM((rows, dim), bf16), pltpu.VMEM((rows, dim), bf16)),
            in_specs=[anywhere] * 6,
            out_specs=(in_vmem, in_vmem, in_vmem),
            scratch_shapes=[
                pltpu.VMEM(per_head, bf16),
                pltpu.VMEM(per_head, bf16),
                pltpu.VMEM(per_head, bf16),
                pltpu.VMEM((heads, rows), f32),
                pltpu.VMEM((n_dev, 2, 2, half, dim), bf16),
                pltpu.VMEM((heads, dim, rows), bf16),
                pltpu.VMEM((heads, dim, rows), bf16),
                pltpu.VMEM(per_head, f32),
                pltpu.VMEM(per_head, f32),
                pltpu.VMEM(per_head, f32),
                pltpu.VMEM((n_dev, 2, 2, dim, half), f32),
                pltpu.VMEM((2, rows, rows), bf16),
                pltpu.VMEM((2, rows, rows), bf16),
                pltpu.VMEM((n_chips, 2, 2, dim, half), f32),
                pltpu.VMEM((n_chips - 1, 2, 2, dim, half), f32),
                dma((11,)),
                dma((n_chips, 2)),
                dma((n_chips - 1, 2)),
                dma((n_dev, 2)),
                dma((n_chips, 2)),
                dma((n_chips, 2)),
                dma((n_chips - 1, 2)),
                dma((n_chips - 1, 2)),
            ],
            compiler_params=pltpu.CompilerParams(collective_id=0, has_side_effects=True, vmem_limit_bytes=40 * 2**20),
            name='attention_grad',
        )(*[pltpu.with_memory_space_constraint(operand, pltpu.HBM) for operand in operands])
        grad_q, grad_k, grad_v = pl.pallas_call(
            store_kernel,
            out_shape=[jax.ShapeDtypeStruct(grad.shape, bf16) for grad in grads],
            in_specs=[in_vmem] * 3,
            out_specs=[anywhere] * 3,
            scratch_shapes=[dma((3,))],
            compiler_params=pltpu.CompilerParams(vmem_limit_bytes=2**20),
            name='store_grads',
        )(*grads)
        return grad_q.transpose(1, 0, 2), grad_k, grad_v

    return jax.shard_map(local_fn, mesh=mesh, in_specs=(row_spec,) * 6, out_specs=(row_spec,) * 3, check_vma=False)
```

```python
import functools

import jax
import jax.numpy as jnp
from jax import lax
from jax.experimental import pallas as pl
from jax.experimental.pallas import tpu as pltpu
from jax.sharding import PartitionSpec as P

LOG2E = 1.4426950408889634
MESH = pl.DeviceIdType.MESH
NT = ((1,), (1,))
NN = ((1,), (0,))


def dot(lhs, rhs, dims):
    return lax.dot_general(lhs, rhs, (dims, ((), ())), preferred_element_type=jnp.float32)


def wide(column, width):
    return jnp.concatenate([column] * (width // column.shape[1]), axis=1)


def attention_kernel(n_dev, softmax_scale, q_hbm, k_hbm, v_hbm, o_hbm, do_hbm, lse_hbm, dq_ref, dk_ref, dv_ref,
                     q_ref, do_ref, o_ref, lse_ref, kv_ref, q_t, do_t, lse_col, delta_col, dq_acc, acc, p_buf, s_buf,
                     from_core, from_chip,
                     load_sem, own_send, forward_send, kv_recv, core_send, core_recv, chip_send, chip_recv):
    heads, rows, dim = q_ref.shape
    half = rows // 2
    n_chips = n_dev // 2
    local = n_chips - 1
    me = lax.axis_index('cp')
    chip, core = me // 2, lax.rem(me, 2)
    partner = 2 * chip + 1 - core
    log_scale = softmax_scale * LOG2E

    barrier = pltpu.get_barrier_semaphore()
    for step in range(1, n_dev):
        pl.semaphore_signal(barrier, inc=1, device_id={'cp': lax.rem(me + step, n_dev)}, device_id_type=MESH)

    kv_loads = []
    for part in range(2):
        on_part = pl.ds(part * half, half)
        kv_loads.append(pltpu.make_async_copy(k_hbm.at[on_part], kv_ref.at[me, part, 0], load_sem.at[2 * part]))
        kv_loads.append(pltpu.make_async_copy(v_hbm.at[on_part], kv_ref.at[me, part, 1], load_sem.at[2 * part + 1]))
    early = heads // 3

    def head_loads(at, count, sem):
        on_heads = pl.ds(at, count)
        pairs = ((q_hbm, q_ref), (do_hbm, do_ref), (o_hbm, o_ref))
        return [pltpu.make_async_copy(src.at[on_heads], dst.at[on_heads], load_sem.at[sem + n]) for n, (src, dst) in enumerate(pairs)]

    first_loads = [pltpu.make_async_copy(lse_hbm, lse_ref, load_sem.at[4])] + head_loads(0, early, 5)
    later_loads = head_loads(early, heads - early, 8)
    for load in kv_loads + first_loads + later_loads:
        load.start()

    def remote(src, dst, send, recv, target):
        return pltpu.make_async_remote_copy(src_ref=src, dst_ref=dst, send_sem=send, recv_sem=recv, device_id={'cp': target}, device_id_type=MESH)

    def round_of(turn, side):
        late, odd = turn // 2, lax.rem(turn, 2)
        flip = jnp.where(turn == 4, side, 1 - side)
        last_owner = jnp.where(turn == 0, 2, jnp.where(turn < 3, 1, jnp.where(turn == 3, 0, 2 * flip)))
        last_part = jnp.where((turn == 2) | (turn >= 4), 1, 0)
        is_last = chip == n_chips - 1
        return jnp.where(is_last, last_owner, late), jnp.where(is_last, last_part, odd)

    def kv_to_chip(far, part):
        return remote(kv_ref.at[me, part], kv_ref.at[me, part], own_send.at[far, part], kv_recv.at[me, part], me + 2 * far)

    def kv_to_partner(part):
        return remote(kv_ref.at[me, part], kv_ref.at[me, part], own_send.at[0, part], kv_recv.at[me, part], partner)

    def kv_forward(owner, part):
        block = 2 * owner + core
        return remote(kv_ref.at[block, part], kv_ref.at[block, part], forward_send.at[owner, part], kv_recv.at[block, part], partner)

    def wait_kv(block, part):
        remote(kv_ref.at[block, part], kv_ref.at[block, part], own_send.at[0, part], kv_recv.at[block, part], partner).wait_recv()

    def receive(turn):
        owner, part = round_of(turn, core)
        wait_kv(2 * owner + core, part)
        kv_forward(owner, part).start()

    def sum_to_partner(block, slot, part):
        return remote(acc.at[block, part], from_core.at[slot, part], core_send.at[slot, part], core_recv.at[slot, part], partner)

    def sum_to_owner(owner, part):
        block, slot = 2 * owner + core, chip - owner - 1
        target = jnp.where(slot == 1, 2 * (2 * n_chips - 3 - chip) + core, block)
        return remote(acc.at[block, part], from_chip.at[slot, part], chip_send.at[owner, part], chip_recv.at[slot, part], target)

    def wait_sum(slot, part):
        remote(acc.at[me, part], from_chip.at[slot, part], chip_send.at[0, part], chip_recv.at[slot, part], partner).wait_recv()

    def merge(turn):
        owner, part = round_of(turn, core)
        block = 2 * owner + core
        sum_to_partner(block, owner, part).wait_recv()
        acc[block, part] += from_core[owner, part]

        @pl.when((chip >= 2) & (chip + owner == n_chips - 1))
        def _():
            wait_sum(1, part)
            acc[block, part] += from_chip[1, part]

        sum_to_owner(owner, part).start()

    def on_later_chips(action, fars):
        for far in fars:
            @pl.when(chip + far < n_chips)
            def _():
                for part in range(2):
                    action(far, part)

    for load in kv_loads:
        load.wait()
    pl.semaphore_wait(barrier, n_dev - 1)
    on_later_chips(lambda far, part: kv_to_chip(far, part).start(), range(n_chips - 2, 0, -1))

    @pl.when(core == 0)
    def _():
        for part in range(2):
            kv_to_partner(part).start()

    for load in first_loads:
        load.wait()

    def prepare(head):
        if head == early:
            for load in later_loads:
                load.wait()
        at = head + me // n_dev
        q_t[at] = q_ref[head].T
        do_t[at] = do_ref[head].T
        lse_col[at] = jnp.broadcast_to(lse_ref[pl.ds(at, 1), :] * LOG2E, (dim, rows)).T
        delta = jnp.sum(do_ref[head].astype(jnp.float32) * o_ref[head].astype(jnp.float32), axis=1, keepdims=True)
        delta_col[at] = jnp.broadcast_to(delta, (rows, dim))

    def tile(block, part, head, slot, row_at, col_at, diagonal):
        on_rows, on_cols = slice(row_at, row_at + half), slice(col_at, col_at + half)
        prob = jnp.exp2(dot(q_ref[head, on_rows], kv_ref[block, part, 0], NT) * log_scale - wide(lse_col[head, on_rows], half))
        if diagonal:
            row_ids = lax.broadcasted_iota(jnp.int32, prob.shape, 0)
            col_ids = lax.broadcasted_iota(jnp.int32, prob.shape, 1)
            prob = jnp.where(col_ids <= row_ids, prob, 0.0)
        d_prob = dot(do_ref[head, on_rows], kv_ref[block, part, 1], NT)
        score = prob * (d_prob - wide(delta_col[head, on_rows], half))
        p_buf[slot, on_rows, on_cols] = prob.astype(jnp.bfloat16)
        s_buf[slot, on_rows, on_cols] = score.astype(jnp.bfloat16)

    def add_to(ref, index, value, first):
        if first:
            ref[index] = value
        else:
            ref[index] += value

    def add_sums(block, part, head, slot, row_at, col_at):
        on_rows, on_cols = slice(row_at, rows), slice(col_at, col_at + half)
        add_to(acc, (block, part, 1), dot(do_t[head, :, on_rows], p_buf[slot, on_rows, on_cols], NN), head == 0)
        add_to(acc, (block, part, 0), dot(q_t[head, :, on_rows], s_buf[slot, on_rows, on_cols], NN), head == 0)

    def keys(block):
        return jnp.concatenate([kv_ref[block, 0, 0], kv_ref[block, 1, 0]], axis=0)

    def staggered(make, use):
        for step in range(heads + 1):
            if step < heads:
                make(step, step % 2)
            if step >= 1:
                use(step - 1, (step - 1) % 2)

    def own_block(block):
        def make(head, slot):
            tile(block, 0, head, slot, 0, 0, True)
            tile(block, 0, head, slot, half, 0, False)
            tile(block, 1, head, slot, half, half, True)
            if head + 1 < heads:
                prepare(head + 1)

        def use(head, slot):
            add_sums(block, 0, head, slot, 0, 0)
            add_sums(block, 1, head, slot, half, half)
            dq_acc[head, 0:half] = dot(s_buf[slot, 0:half, 0:half], kv_ref[block, 0, 0], NN)
            dq_acc[head, half:rows] = dot(s_buf[slot, half:rows, :], keys(block), NN)

        prepare(0)
        staggered(make, use)

    def half_block(block, part):
        def make(head, slot):
            tile(block, part, head, slot, 0, 0, False)
            tile(block, part, head, slot, half, 0, False)

        def use(head, slot):
            add_sums(block, part, head, slot, 0, 0)
            dq_acc[head] += dot(s_buf[slot, :, 0:half], kv_ref[block, part, 0], NN)

        staggered(make, use)

    own_block(me)
    on_later_chips(lambda far, part: kv_to_chip(far, part).start(), [n_chips - 1])

    def core_block(part):
        wait_kv(2 * chip, part)
        half_block(2 * chip, part)
        sum_to_partner(2 * chip, local, part).start()

    def visit(visit_id, _):
        turn, second = visit_id // 2, lax.rem(visit_id, 2)
        mine = jnp.where(turn < 2, 1 - second, second)
        side = jnp.where(mine == 1, core, 1 - core)
        owner, part = round_of(turn, side)
        block = 2 * owner + side

        @pl.when((turn < 2) & (second == 0))
        def _():
            receive(turn)

        @pl.when((turn >= 1) & (second == 1) & (turn + 1 < 2 * chip))
        def _():
            receive(turn + 1)

        @pl.when(mine == 0)
        def _():
            wait_kv(block, part)

        half_block(block, part)

        @pl.when(mine == 0)
        def _():
            sum_to_partner(block, owner, part).start()

        @pl.when((turn >= 1) & (turn <= 3) & (second == 0))
        def _():
            merge(turn - 1)

        @pl.when((second == 1) & ((turn >= 3) | ((turn == 1) & (chip == 1))))
        def _():
            merge(turn)

        return 0

    lax.fori_loop(0, 4 * chip, visit, 0)

    @pl.when(core == 1)
    def _():
        core_block(0)
        core_block(1)

    for head in range(heads):
        dq_ref[head] = (dq_acc[head] * softmax_scale).astype(jnp.bfloat16)

    @pl.when(core == 0)
    def _():
        for part in range(2):
            sum_to_partner(me, local, part).wait_recv()
        acc[me] += from_core[local]

    for part in range(2):
        on_part = slice(part * half, (part + 1) * half)
        for far in (1, n_chips - 1):
            @pl.when(chip + far < n_chips)
            def _():
                wait_sum(far - 1, part)
                acc[me, part] += from_chip[far - 1, part]

        dk_ref[on_part] = (acc[me, part, 0] * softmax_scale).T.astype(jnp.bfloat16)
        dv_ref[on_part] = acc[me, part, 1].T.astype(jnp.bfloat16)

    on_later_chips(lambda far, part: kv_to_chip(far, part).wait_send(), range(1, n_chips))

    @pl.when(core == 0)
    def _():
        for part in range(2):
            kv_to_partner(part).wait_send()

    @pl.when(core == 1)
    def _():
        for part in range(2):
            sum_to_partner(2 * chip, local, part).wait_send()

    def finish(owner, _):
        for part in range(2):
            kv_forward(owner, part).wait_send()
            sum_to_partner(2 * owner + 1 - core, owner, part).wait_send()
            sum_to_owner(owner, part).wait_send()
        return 0

    lax.fori_loop(0, chip, finish, 0)


def store_kernel(dq_ref, dk_ref, dv_ref, dq_hbm, dk_hbm, dv_hbm, sem):
    stores = [
        pltpu.make_async_copy(dq_ref, dq_hbm, sem.at[0]),
        pltpu.make_async_copy(dk_ref, dk_hbm, sem.at[1]),
        pltpu.make_async_copy(dv_ref, dv_hbm, sem.at[2]),
    ]
    for store in stores:
        store.start()
    for store in stores:
        store.wait()


def solution(mesh):
    n_dev = mesh.shape['cp']
    n_chips = n_dev // 2
    row_spec = P(('dp', 'cp'))
    f32, bf16 = jnp.float32, jnp.bfloat16

    def local_fn(q_tok, k_tok, v_tok, fwd_out, d_out, lse_row):
        rows, heads, dim = q_tok.shape
        half = rows // 2
        per_head = (heads, rows, dim)
        anywhere = pl.BlockSpec(memory_space=pl.ANY)
        in_vmem = pl.BlockSpec(memory_space=pltpu.VMEM)
        dma = pltpu.SemaphoreType.DMA
        operands = (q_tok.transpose(1, 0, 2), k_tok, v_tok, fwd_out.transpose(1, 0, 2), d_out.transpose(1, 0, 2), lse_row.T)
        grads = pl.pallas_call(
            functools.partial(attention_kernel, n_dev, dim ** -0.5),
            out_shape=(pltpu.VMEM(per_head, bf16), pltpu.VMEM((rows, dim), bf16), pltpu.VMEM((rows, dim), bf16)),
            in_specs=[anywhere] * 6,
            out_specs=(in_vmem, in_vmem, in_vmem),
            scratch_shapes=[
                pltpu.VMEM(per_head, bf16),
                pltpu.VMEM(per_head, bf16),
                pltpu.VMEM(per_head, bf16),
                pltpu.VMEM((heads, rows), f32),
                pltpu.VMEM((n_dev, 2, 2, half, dim), bf16),
                pltpu.VMEM((heads, dim, rows), bf16),
                pltpu.VMEM((heads, dim, rows), bf16),
                pltpu.VMEM(per_head, f32),
                pltpu.VMEM(per_head, f32),
                pltpu.VMEM(per_head, f32),
                pltpu.VMEM((n_dev, 2, 2, dim, half), f32),
                pltpu.VMEM((2, rows, rows), bf16),
                pltpu.VMEM((2, rows, rows), bf16),
                pltpu.VMEM((n_chips, 2, 2, dim, half), f32),
                pltpu.VMEM((n_chips - 1, 2, 2, dim, half), f32),
                dma((11,)),
                dma((n_chips, 2)),
                dma((n_chips - 1, 2)),
                dma((n_dev, 2)),
                dma((n_chips, 2)),
                dma((n_chips, 2)),
                dma((n_chips - 1, 2)),
                dma((n_chips - 1, 2)),
            ],
            compiler_params=pltpu.CompilerParams(collective_id=0, has_side_effects=True, vmem_limit_bytes=40 * 2**20),
            name='attention_grad',
        )(*[pltpu.with_memory_space_constraint(operand, pltpu.HBM) for operand in operands])
        grad_q, grad_k, grad_v = pl.pallas_call(
            store_kernel,
            out_shape=[jax.ShapeDtypeStruct(grad.shape, bf16) for grad in grads],
            in_specs=[in_vmem] * 3,
            out_specs=[anywhere] * 3,
            scratch_shapes=[dma((3,))],
            compiler_params=pltpu.CompilerParams(vmem_limit_bytes=2**20),
            name='store_grads',
        )(*grads)
        return grad_q.transpose(1, 0, 2), grad_k, grad_v

    return jax.shard_map(local_fn, mesh=mesh, in_specs=(row_spec,) * 6, out_specs=(row_spec,) * 3, check_vma=False)
```
